32 devices in a mesh: blk: 16 (over z, y, core), along: 2 (over x).
Axes of the slice: x: 2, y: 2, z: 4, core: 2. Of those that a mesh axis runs over, the one named last changes fastest.
Arguments:
- values: float32 [3, 16, 48, 256], P(None, 'blk', 'along'), may hold values from -6 to 6
- offsets: float32 [3, 16, 48, 256], P(None, 'blk', 'along'), may hold values from 0 to 1
- stiffness: float32 [16, 48, 256], P('blk', 'along'), may hold values from 0.5 to 2
- leaf_basis: float32 [16, 48, 64, 256], P('blk', 'along'), may hold values from -0.375 to 0.375
- transfer: float32 [16, 48, 64, 64], P('blk', 'along'), may hold values from -0.15625 to 0.15625
- slab_transfer_matrices: float32 [16, 2, 64, 64], P('blk', 'along'), may hold values from -0.5 to 0.5
- leaf_coupling_matrices: float32 [16, 30, 64, 64], P('blk'), may hold values from -0.375 to 0.375
- leaf_admissible_mask: int32 [16, 30], P('blk'), may hold values 0 or 1
- top_coupling: float32 [16, 16, 64, 64], P('blk'), may hold values from -0.75 to 0.75
- top_admissible: int32 [16, 16], P('blk'), may hold values 0 or 1
Outputs:
- product: float32 [3, 16, 48, 256], P(None, 'blk', 'along')
The draws below stay inside these ranges and needn't reach their ends.
All inputs are finite; a program needn't handle non-finite values. No bound on the sum of `leaf_admissible_mask` or of `top_admissible` on one device may be relied on, other than what follows from the above.
Results may differ from the reference program's by a relative error of at most 0.0001.
Values sent between devices are 32-bit elements; how exact they have to be, the bound alone decides.
A program may use at most 64 MiB of HBM per device.

```python
import math
import jax
import jax.numpy as jnp
from jax import lax

LEAF = 256
BASIS_RANK = 64
RHS = 3
LD = 24
REACH = 6
SECTOR_COUNT = 16
NAX = 48
SLOT_COUNT = 30


def set_ends(array, key, least, high):
    index_at = [jax.random.randint(jax.random.fold_in(key, axis), (), 0, length) for axis, length in enumerate(array.shape)]
    longest = array.shape.index(max(array.shape))
    next_to = index_at[:longest] + [(index_at[longest] + 1) % array.shape[longest]] + index_at[longest + 1:]
    return array.at[tuple(index_at)].set(least).at[tuple(next_to)].set(high)


def steps_of(rng, shape, cuts, low, high):
    def one(axis_at, parts):
        draws = jax.random.uniform(jax.random.fold_in(jax.random.fold_in(rng, 6), axis_at), (parts,), jnp.float32, low / len(cuts), high / len(cuts))
        return jnp.repeat(jnp.exp(draws), shape[axis_at] // parts).reshape((-1,) + (1,) * (len(shape) - axis_at - 1))

    gain = one(*cuts[0])
    for cut in cuts[1:]:
        gain = gain * one(*cut)
    return gain


def bell_draw(rng, dims, deviation, limit, split=(), held_as=jnp.bfloat16):
    entries = deviation * jax.random.normal(rng, dims, jnp.float32)
    if split:
        entries = entries * steps_of(rng, dims, split, -0.22, 0.18)
    return jnp.clip(entries, -limit, limit).astype(held_as)


def setup_inputs(seed: int = 0) -> dict:
    keys = jax.random.split(jax.random.key(seed), 11)
    values = bell_draw(keys[0], (RHS, SECTOR_COUNT, NAX, LEAF), 1.0, 6.0, ((1, 16), (2, 2)), jnp.float32)
    offsets = jnp.clip(1.0 * jax.random.uniform(keys[1], (3, SECTOR_COUNT, NAX, LEAF), jnp.float32) ** steps_of(keys[1], (3, SECTOR_COUNT, NAX, LEAF), ((1, 16), (2, 2)), -0.2, 0.2), 0.0, 1.0)
    stiffness = jnp.clip(jnp.exp(math.log(2.0) - 1.3862944 * jax.random.uniform(keys[2], (SECTOR_COUNT, NAX, LEAF), jnp.float32) ** steps_of(keys[2], (SECTOR_COUNT, NAX, LEAF), ((0, 16), (1, 2)), -0.2, 0.2)), 0.5, 2.0)
    leaf_basis = bell_draw(keys[3], (SECTOR_COUNT, NAX, BASIS_RANK, LEAF), LEAF ** -0.5, 0.375, ((0, 16), (1, 2)), jnp.float32)
    transfer = bell_draw(keys[4], (SECTOR_COUNT, NAX, BASIS_RANK, BASIS_RANK), (BASIS_RANK * LD) ** -0.5, 0.15625, ((0, 16), (1, 2)), jnp.float32)
    slab_transfer_matrices = bell_draw(keys[5], (SECTOR_COUNT, NAX // LD, BASIS_RANK, BASIS_RANK), (BASIS_RANK * NAX // LD) ** -0.5, 0.5, ((0, 16), (1, 2)), jnp.float32)
    leaf_coupling_matrices = bell_draw(keys[6], (SECTOR_COUNT, SLOT_COUNT, BASIS_RANK, BASIS_RANK), (4 * BASIS_RANK) ** -0.5, 0.375, ((0, 16),), jnp.float32)
    leaf_admissible_mask = set_ends((jax.random.randint(keys[7], (SECTOR_COUNT, SLOT_COUNT), 0, 4) < 3).astype(jnp.int32), jax.random.fold_in(keys[7], 1), 0, 1)
    top_coupling = bell_draw(keys[8], (SECTOR_COUNT, SECTOR_COUNT, BASIS_RANK, BASIS_RANK), BASIS_RANK ** -0.5, 0.75, ((0, 16),), jnp.float32)
    top_admissible = set_ends((jax.random.randint(keys[9], (SECTOR_COUNT, SECTOR_COUNT), 0, 4) < 3).astype(jnp.int32), jax.random.fold_in(keys[9], 1), 0, 1)
    return {"values": values, "offsets": offsets, "stiffness": stiffness, "leaf_basis": leaf_basis, "transfer": transfer, "slab_transfer_matrices": slab_transfer_matrices, "leaf_coupling_matrices": leaf_coupling_matrices, "leaf_admissible_mask": leaf_admissible_mask, "top_coupling": top_coupling, "top_admissible": top_admissible}


SHARPNESS = 2.0
KERNEL_SCALE = 0.125
HIGHEST_ACCURACY = lax.Precision.HIGHEST


def near_field(padded):
    leaves = padded.shape[2] - 2
    center = padded[:, 1:2, 1:1 + leaves]
    result = jnp.zeros((3, 1, leaves, padded.shape[3]), jnp.float32)
    for around in (-1, 0, 1):
        for along_step in (-1, 0, 1):
            source = padded[:, 1 + around:2 + around, 1 + along_step:1 + along_step + leaves]
            gap_around = around + source[0][..., None, :] - center[0][..., :, None]
            gap_along = along_step + source[1][..., None, :] - center[1][..., :, None]
            gap_radial = source[2][..., None, :] - center[2][..., :, None]
            squared = gap_around * gap_around + gap_along * gap_along + gap_radial * gap_radial
            kernel = KERNEL_SCALE * center[3][..., :, None] * source[3][..., None, :] * jnp.exp(-SHARPNESS * squared)
            result = result + jnp.einsum('alij,ralj->rali', kernel, source[4:], precision=HIGHEST_ACCURACY)
    return result


def slot_number(around, along_step, reach):
    block = around - 2 if around > 0 else reach - 1 + (-around - 2)
    return 3 * block + along_step + 1


def reference(values, offsets, stiffness, leaf_basis, transfer, slab_transfer_matrices, leaf_coupling_matrices, leaf_admissible_mask, top_coupling, top_admissible):
    stacked = jnp.concatenate([offsets, stiffness[None], values], 0)
    stacked = jnp.pad(stacked, ((0, 0), (0, 0), (1, 1), (0, 0)))
    stacked = jnp.concatenate([stacked[:, -1:], stacked, stacked[:, :1]], 1)

    def one_sector(sector):
        block = lax.dynamic_slice_in_dim(stacked, sector, 3, 1)
        return near_field(block)[:, 0]

    near = lax.map(one_sector, jnp.arange(SECTOR_COUNT, dtype=jnp.int32))
    near = jnp.transpose(near, (1, 0, 2, 3))

    coefs = jnp.einsum('slki,rsli->rslk', leaf_basis, values, precision=HIGHEST_ACCURACY)
    padded_coefs = jnp.pad(coefs, ((0, 0), (0, 0), (1, 1), (0, 0)))
    far_leaf = jnp.zeros(coefs.shape, jnp.float32)
    offsets_list = list(range(2, REACH + 1)) + [-step for step in range(2, REACH + 1)]
    for around in offsets_list:
        rolled = jnp.roll(padded_coefs, -around, axis=1)
        for along_step in (-1, 0, 1):
            slot = slot_number(around, along_step, REACH)
            partner = rolled[:, :, 1 + along_step:1 + along_step + NAX]
            coupling = leaf_coupling_matrices[:, slot] * leaf_admissible_mask[:, slot].astype(jnp.float32)[:, None, None]
            far_leaf = far_leaf + jnp.einsum('skq,rslq->rslk', coupling, partner, precision=HIGHEST_ACCURACY)

    slabs = NAX // LD
    grouped = coefs.reshape(RHS, SECTOR_COUNT, slabs, LD, BASIS_RANK)
    links = transfer.reshape(SECTOR_COUNT, slabs, LD, BASIS_RANK, BASIS_RANK)
    slab_coefficient_rows = jnp.einsum('splqk,rsplq->rspk', links, grouped, precision=HIGHEST_ACCURACY)
    sector_coefs = jnp.einsum('spqk,rspq->rsk', slab_transfer_matrices, slab_coefficient_rows, precision=HIGHEST_ACCURACY)

    indices = jnp.arange(SECTOR_COUNT, dtype=jnp.int32)
    apart = (indices[None, :] - indices[:, None]) % SECTOR_COUNT
    distant = jnp.logical_and(apart > REACH, apart < SECTOR_COUNT - REACH).astype(jnp.float32)
    allowed = top_admissible.astype(jnp.float32) * distant
    sector_local_coefs = jnp.einsum('stkq,rtq->rsk', top_coupling * allowed[:, :, None, None], sector_coefs, precision=HIGHEST_ACCURACY)

    slab_local_coefs = jnp.einsum('spqk,rsk->rspq', slab_transfer_matrices, sector_local_coefs, precision=HIGHEST_ACCURACY)
    leaf_down = jnp.einsum('splqk,rspk->rsplq', links, slab_local_coefs, precision=HIGHEST_ACCURACY).reshape(RHS, SECTOR_COUNT, NAX, BASIS_RANK)
    leaf_local = far_leaf + leaf_down
    return near + jnp.einsum('slki,rslk->rsli', leaf_basis, leaf_local, precision=HIGHEST_ACCURACY)
```

```python
import jax
import jax.numpy as jnp
from jax import lax
from jax.experimental import pallas as pl
from jax.experimental.pallas import tpu as pltpu
from jax.sharding import PartitionSpec as P

REACH = 6


SHARPNESS = 2.0
KERNEL_SCALE = 0.125
HIGHEST_ACCURACY = lax.Precision.HIGHEST


def with_halo(cells, sides, width, closed):
    for axis, dim in sides:
        count = lax.axis_size(axis)
        ends = count if closed else count - 1
        head = lax.slice_in_dim(cells, 0, width, axis=dim)
        tail = lax.slice_in_dim(cells, cells.shape[dim] - width, cells.shape[dim], axis=dim)
        cells = jnp.concatenate(
            [
                lax.ppermute(tail, axis, [(i, (i + 1) % count) for i in range(ends)]),
                cells,
                lax.ppermute(head, axis, [((i + 1) % count, i) for i in range(ends)]),
            ],
            axis=dim,
        )
    return cells


def passed_along(x, axis, by):
    count = lax.axis_size(axis)
    return lax.ppermute(x, axis, [(i, (i + by) % count) for i in range(count)])


def split_in_two(x):
    high = x.astype(jnp.bfloat16).astype(jnp.float32)
    return high, x - high


def near_kernel(cells_ref, out_ref, feature_ref, weight_ref):
    leaves, _, size = out_ref.shape
    row = lax.broadcasted_iota(jnp.int32, (8, size), 0)
    log2e = 1.4426950408889634

    def prepare(a):
        def step(m, carry):
            cell = cells_ref[a, m]
            high, low = split_in_two(jnp.where(row < 3, cell, 0.0))
            stacked = jnp.concatenate([high, low, high, low], 0)
            feature_ref[a, m] = stacked.T.astype(jnp.bfloat16)
            around = cell[0:1] + (a - 1.0)
            radial = cell[2:3]
            part = around * around + radial * radial
            for b in range(3):
                along = cell[1:2] + (b - 1.0)
                factor = jnp.exp2((-SHARPNESS * log2e) * (part + along * along))
                high, low = split_in_two(cell * factor)
                weight_ref[a, m, b] = jnp.concatenate([high, low], 0).astype(jnp.bfloat16)
            return carry

        lax.fori_loop(0, leaves + 2, step, 0)

    for a in range(3):
        prepare(a)

    def leaf(m, carry):
        cell = cells_ref[1, m + 1]
        high, low = split_in_two(jnp.where(row < 3, cell * (2 * SHARPNESS * log2e), 0.0))
        target = jnp.concatenate([high, high, low, low], 0).astype(jnp.bfloat16)
        x0, x1, x2 = cell[0:1], cell[1:2], cell[2:3]
        base = (
            KERNEL_SCALE
            * cell[6:7]
            * jnp.exp2((-SHARPNESS * log2e) * (x0 * x0 + x1 * x1 + x2 * x2))
        )
        total = jnp.zeros((8, size), jnp.float32)
        for a in range(3):
            for b in range(3):
                power = jnp.dot(
                    feature_ref[a, m + b], target, preferred_element_type=jnp.float32
                )
                tile = jnp.exp2(power)
                tile_high = tile.astype(jnp.bfloat16)
                tile_low = (tile - tile_high.astype(jnp.float32)).astype(jnp.bfloat16)
                weight = weight_ref[a, m + b, b]
                got = jnp.dot(weight, tile_high, preferred_element_type=jnp.float32) + jnp.dot(
                    weight, tile_low, preferred_element_type=jnp.float32
                )
                factor = base * jnp.exp2(
                    (2 * SHARPNESS * log2e) * ((a - 1.0) * x0 + (b - 1.0) * x1)
                )
                total = total + factor * (got[:8] + got[8:])
        out_ref[m] = total
        return carry

    lax.fori_loop(0, leaves, leaf, 0)


def near_field(padded):
    leaves = padded.shape[1] - 2
    size = padded.shape[3]
    tiles = 9 * leaves * size * size
    return pl.pallas_call(
        near_kernel,
        out_shape=jax.ShapeDtypeStruct((leaves, 8, size), jnp.float32),
        in_specs=[pl.BlockSpec(memory_space=pltpu.VMEM)],
        out_specs=pl.BlockSpec(memory_space=pltpu.VMEM),
        scratch_shapes=[
            pltpu.VMEM((3, leaves + 2, size, 32), jnp.bfloat16),
            pltpu.VMEM((3, leaves + 2, 3, 16, size), jnp.bfloat16),
        ],
        compiler_params=pltpu.CompilerParams(vmem_limit_bytes=40 * 1024 * 1024),
        cost_estimate=pl.CostEstimate(
            flops=100 * tiles, bytes_accessed=16 * padded.size, transcendentals=tiles
        ),
    )(padded)


def slot_number(around, along_step, reach):
    block = around - 2 if around > 0 else reach - 1 + (-around - 2)
    return 3 * block + along_step + 1


def add_sector(total, held, around, leaf_coupling_matrices, leaf_admissible_mask):
    leaves = total.shape[2]
    for along_step in (-1, 0, 1):
        slot = slot_number(around, along_step, REACH)
        partner = held[:, :, 1 + along_step : 1 + along_step + leaves]
        coupling = (
            leaf_coupling_matrices[:, slot]
            * leaf_admissible_mask[:, slot].astype(jnp.float32)[:, None, None]
        )
        total = total + jnp.einsum("skq,rslq->rslk", coupling, partner, precision=HIGHEST_ACCURACY)
    return total


def body(
    values,
    offsets,
    stiffness,
    leaf_basis,
    transfer,
    slab_transfer_matrices,
    leaf_coupling_matrices,
    leaf_admissible_mask,
    top_coupling,
    top_admissible,
):
    cells = jnp.concatenate(
        [
            offsets - 0.5,
            stiffness[None] * values,
            stiffness[None],
            jnp.zeros_like(stiffness)[None],
        ],
        0,
    ).transpose(1, 2, 0, 3)
    padded = with_halo(cells, (("blk", 0), ("along", 1)), 1, True)
    at_start = lax.axis_index("along") == 0
    at_finish = lax.axis_index("along") == lax.axis_size("along") - 1
    lower_rim = jnp.where(at_start, 0.0, padded[:, :1])
    upper_rim = jnp.where(at_finish, 0.0, padded[:, -1:])
    padded = jnp.concatenate([lower_rim, padded[:, 1:-1], upper_rim], 1)
    near = near_field(padded)[:, 3:6].transpose(1, 0, 2)[:, None]
    coefs = jnp.einsum("slki,rsli->rslk", leaf_basis, values, precision=HIGHEST_ACCURACY)
    rimmed = with_halo(coefs, (("along", 2),), 1, False)
    far_leaf = jnp.zeros(coefs.shape, jnp.float32)
    sectors = lax.axis_size("blk")
    lower_window = rimmed
    upper_window = rimmed
    breadth = 1
    while breadth <= REACH:
        lower_came = passed_along(lower_window, "blk", breadth)
        upper_came = passed_along(upper_window, "blk", -breadth)
        lower_window = jnp.concatenate([lower_window, lower_came], 1)
        upper_window = jnp.concatenate([upper_window, upper_came], 1)
        breadth = 2 * breadth
    for distance in range(2, REACH + 1):
        far_leaf = add_sector(
            far_leaf,
            lower_window[:, distance : distance + 1],
            -distance,
            leaf_coupling_matrices,
            leaf_admissible_mask,
        )
        far_leaf = add_sector(
            far_leaf,
            upper_window[:, distance : distance + 1],
            distance,
            leaf_coupling_matrices,
            leaf_admissible_mask,
        )
    slab_coefficient_rows = jnp.einsum(
        "slqk,rslq->rsk", transfer, coefs, precision=HIGHEST_ACCURACY
    )
    shared_portion = jnp.einsum(
        "oxz,eox->eoz",
        slab_transfer_matrices[:, 0],
        slab_coefficient_rows,
        precision=HIGHEST_ACCURACY,
    )
    sector_coefs = lax.psum(shared_portion, "along")
    every_sector = lax.all_gather(sector_coefs, "blk", axis=1, tiled=True)
    sector = lax.axis_index("blk")
    others = jnp.arange(sectors, dtype=jnp.int32)
    apart = (others - sector) % sectors
    distant = jnp.logical_and(apart > REACH, apart < sectors - REACH).astype(jnp.float32)
    allowed = top_admissible[0].astype(jnp.float32) * distant
    sector_local_coefs = jnp.einsum(
        "stkq,rtq->rsk",
        top_coupling * allowed[None, :, None, None],
        every_sector,
        precision=HIGHEST_ACCURACY,
    )
    slab_local_coefs = jnp.einsum(
        "baz,lbz->lba", slab_transfer_matrices[:, 0], sector_local_coefs, precision=HIGHEST_ACCURACY
    )
    leaf_down = jnp.einsum("slqk,rsk->rslq", transfer, slab_local_coefs, precision=HIGHEST_ACCURACY)
    leaf_local = far_leaf + leaf_down
    return near + jnp.einsum("slki,rslk->rsli", leaf_basis, leaf_local, precision=HIGHEST_ACCURACY)


def solution(mesh):
    return jax.shard_map(
        body,
        mesh=mesh,
        in_specs=(
            P(None, "blk", "along", None),
            P(None, "blk", "along", None),
            P("blk", "along", None),
            P("blk", "along", None, None),
            P("blk", "along", None, None),
            P("blk", "along", None, None),
            P("blk", None, None, None),
            P("blk", None),
            P("blk", None, None, None),
            P("blk", None),
        ),
        out_specs=P(None, "blk", "along", None),
        check_vma=False,
    )
```

```python
import jax
import jax.numpy as jnp
from jax import lax
from jax.experimental import pallas as pl
from jax.experimental.pallas import tpu as pltpu
from jax.sharding import PartitionSpec as P

REACH = 6


SHARPNESS = 2.0
KERNEL_SCALE = 0.125
HIGHEST_ACCURACY = lax.Precision.HIGHEST


def split_in_two(x):
    high = x.astype(jnp.bfloat16).astype(jnp.float32)
    return high, x - high


def near_kernel(cells_ref, out_ref, feature_ref, weight_ref):
    leaves, _, size = out_ref.shape
    row = lax.broadcasted_iota(jnp.int32, (8, size), 0)
    log2e = 1.4426950408889634

    def prepare(a):
        def step(m, carry):
            cell = cells_ref[a, m]
            high, low = split_in_two(jnp.where(row < 3, cell, 0.0))
            stacked = jnp.concatenate([high, low, high, low], 0)
            feature_ref[a, m] = stacked.T.astype(jnp.bfloat16)
            around = cell[0:1] + (a - 1.0)
            radial = cell[2:3]
            part = around * around + radial * radial
            for b in range(3):
                along = cell[1:2] + (b - 1.0)
                factor = jnp.exp2((-SHARPNESS * log2e) * (part + along * along))
                high, low = split_in_two(cell * factor)
                weight_ref[a, m, b] = jnp.concatenate([high, low], 0).astype(jnp.bfloat16)
            return carry

        lax.fori_loop(0, leaves + 2, step, 0)

    for a in range(3):
        prepare(a)

    def leaf(m, carry):
        cell = cells_ref[1, m + 1]
        high, low = split_in_two(jnp.where(row < 3, cell * (2 * SHARPNESS * log2e), 0.0))
        target = jnp.concatenate([high, high, low, low], 0).astype(jnp.bfloat16)
        x0, x1, x2 = cell[0:1], cell[1:2], cell[2:3]
        base = (
            KERNEL_SCALE
            * cell[6:7]
            * jnp.exp2((-SHARPNESS * log2e) * (x0 * x0 + x1 * x1 + x2 * x2))
        )
        total = jnp.zeros((8, size), jnp.float32)
        for a in range(3):
            for b in range(3):
                power = jnp.dot(
                    feature_ref[a, m + b], target, preferred_element_type=jnp.float32
                )
                tile = jnp.exp2(power)
                tile_high = tile.astype(jnp.bfloat16)
                tile_low = (tile - tile_high.astype(jnp.float32)).astype(jnp.bfloat16)
                weight = weight_ref[a, m + b, b]
                got = jnp.dot(weight, tile_high, preferred_element_type=jnp.float32) + jnp.dot(
                    weight, tile_low, preferred_element_type=jnp.float32
                )
                factor = base * jnp.exp2(
                    (2 * SHARPNESS * log2e) * ((a - 1.0) * x0 + (b - 1.0) * x1)
                )
                total = total + factor * (got[:8] + got[8:])
        out_ref[m] = total
        return carry

    lax.fori_loop(0, leaves, leaf, 0)


def near_field(padded):
    leaves = padded.shape[1] - 2
    size = padded.shape[3]
    tiles = 9 * leaves * size * size
    return pl.pallas_call(
        near_kernel,
        out_shape=jax.ShapeDtypeStruct((leaves, 8, size), jnp.float32),
        in_specs=[pl.BlockSpec(memory_space=pltpu.VMEM)],
        out_specs=pl.BlockSpec(memory_space=pltpu.VMEM),
        scratch_shapes=[
            pltpu.VMEM((3, leaves + 2, size, 32), jnp.bfloat16),
            pltpu.VMEM((3, leaves + 2, 3, 16, size), jnp.bfloat16),
        ],
        compiler_params=pltpu.CompilerParams(vmem_limit_bytes=40 * 1024 * 1024),
        cost_estimate=pl.CostEstimate(
            flops=100 * tiles, bytes_accessed=16 * padded.size, transcendentals=tiles
        ),
    )(padded)


def far_offsets():
    ahead = list(range(2, REACH + 1))
    return ahead + [-step for step in ahead]


def exchange_kernel(
    cells_ref,
    coefs_ref,
    ends_ref,
    share_ref,
    padded_ref,
    windows_ref,
    rims_ref,
    shares_ref,
    send_sem,
    recv_sem,
    share_send_sem,
    share_recv_sem,
):
    sectors, slabs = lax.axis_size("blk"), lax.axis_size("along")
    sector, slab = lax.axis_index("blk"), lax.axis_index("along")
    leaves = cells_ref.shape[0]
    copies = []

    def send(source, target, around, along):
        k = len(copies)
        copy = pltpu.make_async_remote_copy(
            src_ref=source,
            dst_ref=target,
            send_sem=send_sem.at[k],
            recv_sem=recv_sem.at[k],
            device_id={
                "blk": lax.rem(sector + around + sectors, sectors),
                "along": lax.rem(slab + along + slabs, slabs),
            },
            device_id_type=pl.DeviceIdType.MESH,
        )
        copy.start()
        copies.append(copy)

    distant = sectors - 2 * REACH - 1

    def share_copy(k, row, column):
        return pltpu.make_async_remote_copy(
            src_ref=share_ref,
            dst_ref=shares_ref.at[row, column],
            send_sem=share_send_sem.at[k],
            recv_sem=share_recv_sem.at[k // slabs * slabs + column],
            device_id={
                "blk": lax.rem(sector + REACH + 1 + k // slabs, sectors),
                "along": lax.rem(k, slabs),
            },
            device_id_type=pl.DeviceIdType.MESH,
        )

    def share_start(k, carry):
        share_copy(k, sector, slab).start()
        return carry

    def share_wait(k, carry):
        came = lax.rem(sector + sectors - REACH - 1 - k // slabs, sectors)
        share_copy(k, sector, slab).wait_send()
        share_copy(k, came, lax.rem(k, slabs)).wait_recv()
        return carry

    lax.fori_loop(0, distant * slabs, share_start, 0)
    for around in (-1, 1):
        send(cells_ref, padded_ref.at[1 - around, pl.ds(1, leaves)], around, 0)
    for around in (-1, 0, 1):
        send(cells_ref.at[leaves - 1], padded_ref.at[1 - around, 0], around, 1)
        send(cells_ref.at[0], padded_ref.at[1 - around, leaves + 1], around, -1)
    for q, around in enumerate(far_offsets()):
        send(coefs_ref, windows_ref.at[q], -around, 0)
        send(ends_ref.at[1], rims_ref.at[q, 0], -around, 1)
        send(ends_ref.at[0], rims_ref.at[q, 1], -around, -1)
    padded_ref[1, pl.ds(1, leaves)] = cells_ref[...]
    for copy in copies:
        copy.wait()
    lax.fori_loop(0, distant * slabs, share_wait, 0)

    @pl.when(slab == 0)
    def _():
        padded_ref[:, 0] = jnp.zeros_like(padded_ref[:, 0])
        rims_ref[:, 0] = jnp.zeros_like(rims_ref[:, 0])

    @pl.when(slab == slabs - 1)
    def _():
        padded_ref[:, leaves + 1] = jnp.zeros_like(padded_ref[:, 0])
        rims_ref[:, 1] = jnp.zeros_like(rims_ref[:, 0])


def exchange(cells, coefs, ends, share):
    sectors, slabs = lax.axis_size("blk"), lax.axis_size("along")
    leaves, _, size = cells.shape
    far = 2 * (REACH - 1)
    links = 8 + 3 * far
    pairs = (sectors - 2 * REACH - 1) * slabs
    vmem = pl.BlockSpec(memory_space=pltpu.VMEM)
    return pl.pallas_call(
        exchange_kernel,
        out_shape=(
            jax.ShapeDtypeStruct((3, leaves + 2, 8, size), jnp.float32),
            jax.ShapeDtypeStruct((far, *coefs.shape), jnp.float32),
            jax.ShapeDtypeStruct((far, *ends.shape), jnp.float32),
            jax.ShapeDtypeStruct((sectors, slabs, *share.shape), jnp.float32),
        ),
        in_specs=[vmem] * 4,
        out_specs=(vmem,) * 4,
        scratch_shapes=[
            pltpu.SemaphoreType.DMA((links,)),
            pltpu.SemaphoreType.DMA((links,)),
            pltpu.SemaphoreType.DMA((pairs,)),
            pltpu.SemaphoreType.DMA((pairs,)),
        ],
        compiler_params=pltpu.CompilerParams(has_side_effects=True),
    )(cells, coefs, ends, share)


def body(
    values,
    offsets,
    stiffness,
    leaf_basis,
    transfer,
    slab_transfer_matrices,
    leaf_coupling_matrices,
    leaf_admissible_mask,
    top_coupling,
    top_admissible,
):
    cells = jnp.concatenate(
        [
            offsets - 0.5,
            stiffness[None] * values,
            stiffness[None],
            jnp.zeros_like(stiffness)[None],
        ],
        0,
    ).transpose(1, 2, 0, 3)
    coefs = jnp.einsum("slki,rsli->rslk", leaf_basis, values, precision=HIGHEST_ACCURACY)
    slab_coefficient_rows = jnp.einsum(
        "slqk,rslq->rsk", transfer, coefs, precision=HIGHEST_ACCURACY
    )
    shared_portion = jnp.einsum(
        "oxz,eox->eoz",
        slab_transfer_matrices[:, 0],
        slab_coefficient_rows,
        precision=HIGHEST_ACCURACY,
    )
    by_leaf = coefs[:, 0].transpose(1, 0, 2)
    leaves, count, rank = by_leaf.shape
    width = -(-count * rank // 128) * 128
    lanes = -(-rank // 128) * 128
    flat = by_leaf.reshape(leaves, count * rank)
    ends = jnp.stack([by_leaf[0], by_leaf[-1]])
    padded, windows, rims, shares = exchange(
        cells[0],
        jnp.pad(flat, ((0, 0), (0, width - count * rank))),
        jnp.pad(ends, ((0, 0), (0, 8 - count), (0, lanes - rank))),
        jnp.pad(shared_portion[:, 0], ((0, 8 - count), (0, lanes - rank))),
    )
    near = near_field(padded)[:, 3:6].transpose(1, 0, 2)[:, None]
    far = windows.shape[0]
    windows = windows[:, :, : count * rank].reshape(far, leaves, count, rank)
    rims = rims[:, :, :count, :rank]
    windows = jnp.concatenate([rims[:, :1], windows, rims[:, 1:]], 1)
    partners = jnp.stack([windows[:, b : b + leaves] for b in range(3)], 1)
    coupling = (
        leaf_coupling_matrices[0] * leaf_admissible_mask[0].astype(jnp.float32)[:, None, None]
    ).reshape(far, 3, rank, rank)
    far_leaf = jnp.einsum(
        "qbkz,qblrz->rlk", coupling, partners, precision=HIGHEST_ACCURACY
    )[:, None]
    sectors = lax.axis_size("blk")
    sector = lax.axis_index("blk")
    others = jnp.arange(sectors, dtype=jnp.int32)
    apart = (others - sector) % sectors
    distant = jnp.logical_and(apart > REACH, apart < sectors - REACH)
    allowed = jnp.where(distant, top_admissible[0].astype(jnp.float32), 0.0)
    shares = jnp.where(distant[:, None, None, None], shares, 0.0)
    every_sector = shares.sum(1)[:, :count, :rank].transpose(1, 0, 2)
    sector_local_coefs = jnp.einsum(
        "stkq,rtq->rsk",
        top_coupling * allowed[None, :, None, None],
        every_sector,
        precision=HIGHEST_ACCURACY,
    )
    slab_local_coefs = jnp.einsum(
        "baz,lbz->lba", slab_transfer_matrices[:, 0], sector_local_coefs, precision=HIGHEST_ACCURACY
    )
    leaf_down = jnp.einsum("slqk,rsk->rslq", transfer, slab_local_coefs, precision=HIGHEST_ACCURACY)
    leaf_local = far_leaf + leaf_down
    return near + jnp.einsum("slki,rslk->rsli", leaf_basis, leaf_local, precision=HIGHEST_ACCURACY)


def solution(mesh):
    return jax.shard_map(
        body,
        mesh=mesh,
        in_specs=(
            P(None, "blk", "along", None),
            P(None, "blk", "along", None),
            P("blk", "along", None),
            P("blk", "along", None, None),
            P("blk", "along", None, None),
            P("blk", "along", None, None),
            P("blk", None, None, None),
            P("blk", None),
            P("blk", None, None, None),
            P("blk", None),
        ),
        out_specs=P(None, "blk", "along", None),
        check_vma=False,
    )
```

```python
import functools

import jax
import jax.numpy as jnp
from jax import lax
from jax.experimental import pallas as pl
from jax.experimental.pallas import tpu as pltpu
from jax.sharding import PartitionSpec as P

REACH = 6


SHARPNESS = 2.0
KERNEL_SCALE = 0.125
HIGHEST_ACCURACY = lax.Precision.HIGHEST


def split_in_two(x):
    high = x.astype(jnp.bfloat16).astype(jnp.float32)
    return high, x - high


def near_steps(cells_ref, out_ref, feature_ref, weight_ref):
    leaves, _, size = out_ref.shape
    row = lax.broadcasted_iota(jnp.int32, (8, size), 0)
    log2e = 1.4426950408889634

    def prepare(a):
        def step(m, carry):
            cell = cells_ref[a, m]
            high, low = split_in_two(jnp.where(row < 3, cell, 0.0))
            stacked = jnp.concatenate([high, low, high, low], 0)
            feature_ref[a, m] = stacked.T.astype(jnp.bfloat16)
            around = cell[0:1] + (a - 1.0)
            radial = cell[2:3]
            part = around * around + radial * radial
            for b in range(3):
                along = cell[1:2] + (b - 1.0)
                factor = jnp.exp2((-SHARPNESS * log2e) * (part + along * along))
                high, low = split_in_two(cell * factor)
                weight_ref[a, m, b] = jnp.concatenate([high, low], 0).astype(jnp.bfloat16)
            return carry

        lax.fori_loop(0, leaves + 2, step, 0)

    def leaf(sources, first, m, carry):
        cell = cells_ref[1, m + 1]
        high, low = split_in_two(jnp.where(row < 3, cell * (2 * SHARPNESS * log2e), 0.0))
        target = jnp.concatenate([high, high, low, low], 0).astype(jnp.bfloat16)
        x0, x1, x2 = cell[0:1], cell[1:2], cell[2:3]
        base = (
            KERNEL_SCALE
            * cell[6:7]
            * jnp.exp2((-SHARPNESS * log2e) * (x0 * x0 + x1 * x1 + x2 * x2))
        )
        total = jnp.zeros((8, size), jnp.float32) if first else out_ref[m]
        for a in sources:
            for b in range(3):
                power = jnp.dot(
                    feature_ref[a, m + b], target, preferred_element_type=jnp.float32
                )
                tile = jnp.exp2(power)
                tile_high = tile.astype(jnp.bfloat16)
                tile_low = (tile - tile_high.astype(jnp.float32)).astype(jnp.bfloat16)
                weight = weight_ref[a, m + b, b]
                got = jnp.dot(weight, tile_high, preferred_element_type=jnp.float32) + jnp.dot(
                    weight, tile_low, preferred_element_type=jnp.float32
                )
                factor = base * jnp.exp2(
                    (2 * SHARPNESS * log2e) * ((a - 1.0) * x0 + (b - 1.0) * x1)
                )
                total = total + factor * (got[:8] + got[8:])
        out_ref[m] = total
        return carry

    def run(sources, first):
        for a in sources:
            prepare(a)
        lax.fori_loop(0, leaves, functools.partial(leaf, sources, first), 0)

    return run


def far_offsets():
    ahead = list(range(2, REACH + 1))
    return ahead + [-step for step in ahead]


def exchange_kernel(
    cells_ref,
    coefs_ref,
    ends_ref,
    share_ref,
    near_ref,
    windows_ref,
    rims_ref,
    shares_ref,
    padded_ref,
    feature_ref,
    weight_ref,
    send_sem,
    recv_sem,
    share_send_sem,
    share_recv_sem,
):
    sectors, slabs = lax.axis_size("blk"), lax.axis_size("along")
    sector, slab = lax.axis_index("blk"), lax.axis_index("along")
    leaves = cells_ref.shape[0]
    copies = []

    def send(source, target, around, along):
        k = len(copies)
        copy = pltpu.make_async_remote_copy(
            src_ref=source,
            dst_ref=target,
            send_sem=send_sem.at[k],
            recv_sem=recv_sem.at[k],
            device_id={
                "blk": lax.rem(sector + around + sectors, sectors),
                "along": lax.rem(slab + along + slabs, slabs),
            },
            device_id_type=pl.DeviceIdType.MESH,
        )
        copy.start()
        copies.append(copy)

    distant = sectors - 2 * REACH - 1

    def share_copy(k, row, column):
        return pltpu.make_async_remote_copy(
            src_ref=share_ref,
            dst_ref=shares_ref.at[row, column],
            send_sem=share_send_sem.at[k],
            recv_sem=share_recv_sem.at[k // slabs * slabs + column],
            device_id={
                "blk": lax.rem(sector + REACH + 1 + k // slabs, sectors),
                "along": lax.rem(k, slabs),
            },
            device_id_type=pl.DeviceIdType.MESH,
        )

    def share_start(k, carry):
        share_copy(k, sector, slab).start()
        return carry

    def share_wait(k, carry):
        came = lax.rem(sector + sectors - REACH - 1 - k // slabs, sectors)
        share_copy(k, sector, slab).wait_send()
        share_copy(k, came, lax.rem(k, slabs)).wait_recv()
        return carry

    for around in (0, -1, 1):
        send(cells_ref.at[leaves - 1], padded_ref.at[1 - around, 0], around, 1)
        send(cells_ref.at[0], padded_ref.at[1 - around, leaves + 1], around, -1)
    for around in (-1, 1):
        send(cells_ref, padded_ref.at[1 - around, pl.ds(1, leaves)], around, 0)
    lax.fori_loop(0, distant * slabs, share_start, 0)
    for q, around in enumerate(far_offsets()):
        send(coefs_ref, windows_ref.at[q], -around, 0)
        send(ends_ref.at[1], rims_ref.at[q, 0], -around, 1)
        send(ends_ref.at[0], rims_ref.at[q, 1], -around, -1)
    padded_ref[1, pl.ds(1, leaves)] = cells_ref[...]
    run = near_steps(padded_ref, near_ref, feature_ref, weight_ref)

    def close(a):
        @pl.when(slab == 0)
        def _():
            padded_ref[a, 0] = jnp.zeros_like(padded_ref[a, 0])

        @pl.when(slab == slabs - 1)
        def _():
            padded_ref[a, leaves + 1] = jnp.zeros_like(padded_ref[a, 0])

    for copy in copies[:2]:
        copy.wait()
    close(1)
    run((1,), True)
    for copy in copies[2:8]:
        copy.wait()
    close(0)
    close(2)
    run((0, 2), False)
    for copy in copies[8:]:
        copy.wait()
    lax.fori_loop(0, distant * slabs, share_wait, 0)

    @pl.when(slab == 0)
    def _():
        rims_ref[:, 0] = jnp.zeros_like(rims_ref[:, 0])

    @pl.when(slab == slabs - 1)
    def _():
        rims_ref[:, 1] = jnp.zeros_like(rims_ref[:, 1])


def exchange(cells, coefs, ends, share):
    sectors, slabs = lax.axis_size("blk"), lax.axis_size("along")
    leaves, _, size = cells.shape
    far = 2 * (REACH - 1)
    links = 8 + 3 * far
    pairs = (sectors - 2 * REACH - 1) * slabs
    vmem = pl.BlockSpec(memory_space=pltpu.VMEM)
    return pl.pallas_call(
        exchange_kernel,
        out_shape=(
            jax.ShapeDtypeStruct((leaves, 8, size), jnp.float32),
            jax.ShapeDtypeStruct((far, *coefs.shape), jnp.float32),
            jax.ShapeDtypeStruct((far, *ends.shape), jnp.float32),
            jax.ShapeDtypeStruct((sectors, slabs, *share.shape), jnp.float32),
        ),
        in_specs=[vmem] * 4,
        out_specs=(vmem,) * 4,
        scratch_shapes=[
            pltpu.VMEM((3, leaves + 2, 8, size), jnp.float32),
            pltpu.VMEM((3, leaves + 2, size, 32), jnp.bfloat16),
            pltpu.VMEM((3, leaves + 2, 3, 16, size), jnp.bfloat16),
            pltpu.SemaphoreType.DMA((links,)),
            pltpu.SemaphoreType.DMA((links,)),
            pltpu.SemaphoreType.DMA((pairs,)),
            pltpu.SemaphoreType.DMA((pairs,)),
        ],
        compiler_params=pltpu.CompilerParams(
            has_side_effects=True, vmem_limit_bytes=40 * 1024 * 1024
        ),
    )(cells, coefs, ends, share)


def body(
    values,
    offsets,
    stiffness,
    leaf_basis,
    transfer,
    slab_transfer_matrices,
    leaf_coupling_matrices,
    leaf_admissible_mask,
    top_coupling,
    top_admissible,
):
    cells = jnp.concatenate(
        [
            offsets - 0.5,
            stiffness[None] * values,
            stiffness[None],
            jnp.zeros_like(stiffness)[None],
        ],
        0,
    ).transpose(1, 2, 0, 3)
    coefs = jnp.einsum("slki,rsli->rslk", leaf_basis, values, precision=HIGHEST_ACCURACY)
    slab_coefficient_rows = jnp.einsum(
        "slqk,rslq->rsk", transfer, coefs, precision=HIGHEST_ACCURACY
    )
    shared_portion = jnp.einsum(
        "oxz,eox->eoz",
        slab_transfer_matrices[:, 0],
        slab_coefficient_rows,
        precision=HIGHEST_ACCURACY,
    )
    by_leaf = coefs[:, 0].transpose(1, 0, 2)
    leaves, count, rank = by_leaf.shape
    width = -(-count * rank // 128) * 128
    lanes = -(-rank // 128) * 128
    flat = by_leaf.reshape(leaves, count * rank)
    ends = jnp.stack([by_leaf[0], by_leaf[-1]])
    near, windows, rims, shares = exchange(
        cells[0],
        jnp.pad(flat, ((0, 0), (0, width - count * rank))),
        jnp.pad(ends, ((0, 0), (0, 8 - count), (0, lanes - rank))),
        jnp.pad(shared_portion[:, 0], ((0, 8 - count), (0, lanes - rank))),
    )
    near = near[:, 3:6].transpose(1, 0, 2)[:, None]
    far = windows.shape[0]
    windows = windows[:, :, : count * rank].reshape(far, leaves, count, rank)
    rims = rims[:, :, :count, :rank]
    windows = jnp.concatenate([rims[:, :1], windows, rims[:, 1:]], 1)
    partners = jnp.stack([windows[:, b : b + leaves] for b in range(3)], 1)
    coupling = (
        leaf_coupling_matrices[0] * leaf_admissible_mask[0].astype(jnp.float32)[:, None, None]
    ).reshape(far, 3, rank, rank)
    far_leaf = jnp.einsum(
        "qbkz,qblrz->rlk", coupling, partners, precision=HIGHEST_ACCURACY
    )[:, None]
    sectors = lax.axis_size("blk")
    sector = lax.axis_index("blk")
    others = jnp.arange(sectors, dtype=jnp.int32)
    apart = (others - sector) % sectors
    distant = jnp.logical_and(apart > REACH, apart < sectors - REACH)
    allowed = jnp.where(distant, top_admissible[0].astype(jnp.float32), 0.0)
    shares = jnp.where(distant[:, None, None, None], shares, 0.0)
    every_sector = shares.sum(1)[:, :count, :rank].transpose(1, 0, 2)
    sector_local_coefs = jnp.einsum(
        "stkq,rtq->rsk",
        top_coupling * allowed[None, :, None, None],
        every_sector,
        precision=HIGHEST_ACCURACY,
    )
    slab_local_coefs = jnp.einsum(
        "baz,lbz->lba", slab_transfer_matrices[:, 0], sector_local_coefs, precision=HIGHEST_ACCURACY
    )
    leaf_down = jnp.einsum("slqk,rsk->rslq", transfer, slab_local_coefs, precision=HIGHEST_ACCURACY)
    leaf_local = far_leaf + leaf_down
    return near + jnp.einsum("slki,rslk->rsli", leaf_basis, leaf_local, precision=HIGHEST_ACCURACY)


def solution(mesh):
    return jax.shard_map(
        body,
        mesh=mesh,
        in_specs=(
            P(None, "blk", "along", None),
            P(None, "blk", "along", None),
            P("blk", "along", None),
            P("blk", "along", None, None),
            P("blk", "along", None, None),
            P("blk", "along", None, None),
            P("blk", None, None, None),
            P("blk", None),
            P("blk", None, None, None),
            P("blk", None),
        ),
        out_specs=P(None, "blk", "along", None),
        check_vma=False,
    )
```
